32 devices in a mesh: ao: 8 (over y, x, core), aux: 4 (over z).
Axes of the slice: x: 2, y: 2, z: 4, core: 2. Of those that a mesh axis runs over, the one named last changes fastest.
Arguments:
- blocks: bfloat16 [48, 256, 128, 128], P('ao', 'aux'), may hold values from -6 to 6
- pairs: int32 [48, 2], P('ao'), may hold values from 0 to 79, as said below
- counts: int32 [8], P('ao'), may hold values from 1 to 6, as said below
- owned_blocks: int32 [80], P('ao'), may hold values from 0 to 79, as said below
- occ_coef: bfloat16 [80, 8, 128], P('ao'), may hold values from -0.5 to 0.5
- vir_coef: bfloat16 [10240, 9216], P('ao', 'aux'), may hold values from -0.109375 to 0.109375
Outputs:
- b_tensor: bfloat16 [256, 8, 9216], P('ao', None, 'aux')
The draws below stay inside these ranges and needn't reach their ends.
Inputs may be any that keep to these rules, and one draw needn't show every extreme that they name: `pairs`: among the used slots of one ao index, at most 3 have nu blocks whose rows one owner holds; in every draw some index reaches 3. `counts`: some ao index uses all 6 slots in every draw. `owned_blocks`: every atom block appears exactly once.
All inputs are finite; a program needn't handle non-finite values.
Results may differ from the reference program's by a relative error of at most 0.014.
Values may be sent and summed in bfloat16 or wider, within the bound.
No kernel may reach another device: no remote copies, remote signals or barrier semaphores. Data moves between devices by JAX's collectives and lax.ppermute only.
A program may use at most 128 MiB of HBM per device.

```python
import jax
import jax.numpy as jnp
from jax import lax

BLK = 128
BLK_DEV = 10
OCC = 8
SLOTS = 6
NBLK = 80
NAO = 10240
PS = 256
V = 9216
CAP = 3
ALL_SLOTS = 48
N_AO = 8


def slot_layout(key):
    perm_blocks = jax.random.permutation(jax.random.fold_in(key, 11), NBLK).astype(jnp.int32)
    used_counts = jax.random.randint(jax.random.fold_in(key, 12), (N_AO,), 1, SLOTS + 1).astype(jnp.int32)
    full_index = jax.random.randint(jax.random.fold_in(key, 13), (), 0, N_AO)
    used_counts = jnp.where(jnp.arange(N_AO) == full_index, SLOTS, used_counts).astype(jnp.int32)
    first_owner = jax.random.randint(jax.random.fold_in(key, 14), (N_AO,), 0, N_AO)
    second_owner = (first_owner + 1 + jax.random.randint(jax.random.fold_in(key, 15), (N_AO,), 0, N_AO - 1)) % N_AO
    slot_half = jnp.arange(SLOTS) // CAP
    owner_pick = jnp.where(slot_half[None, :] == 0, first_owner[:, None], second_owner[:, None])
    local_pick = jax.random.randint(jax.random.fold_in(key, 16), (N_AO, SLOTS), 0, BLK_DEV)
    second_block = perm_blocks[owner_pick * BLK_DEV + local_pick]
    first_block = jax.random.randint(jax.random.fold_in(key, 17), (N_AO, SLOTS), 0, NBLK)
    pair_list = jnp.stack([first_block, second_block], axis=-1).reshape(N_AO * SLOTS, 2).astype(jnp.int32)
    return (pair_list, used_counts, perm_blocks)


def draw_pairs(key, part):
    return slot_layout(key)[0]


def draw_counts(key, part):
    return slot_layout(key)[1]


def draw_owned_blocks(key, part):
    return slot_layout(key)[2]


def steps_of(stream_key, extent, shards, low, top_value):
    factor_of, own = 1.0, jax.random.fold_in(stream_key, 6)
    for axis_at, shards_of in shards:
        draws = jnp.exp(jax.random.uniform(jax.random.fold_in(own, axis_at), (shards_of,), jnp.float32, low / len(shards), top_value / len(shards)))
        factor_of = factor_of * jnp.repeat(draws, extent[axis_at] // shards_of).reshape([-1 if axis == axis_at else 1 for axis in range(len(extent))])
    return factor_of


def scatter_about(rng, shape, width, bound, pieces=(), kind=jnp.bfloat16):
    array = jax.random.normal(rng, shape, jnp.float32) * width
    if len(pieces) > 0:
        array = steps_of(rng, shape, pieces, -0.22, 0.18) * array
    return jnp.clip(array, min=-bound, max=bound).astype(kind)


def setup_inputs(seed: int = 0) -> dict:
    streams_of = jax.random.split(jax.random.key(seed), 7)
    blocks = scatter_about(streams_of[0], (ALL_SLOTS, PS, BLK, BLK), 1.0, 6.0, ((0, 8), (1, 4)))
    pairs = draw_pairs(jax.random.fold_in(streams_of[6], 71), 0)
    counts = draw_counts(jax.random.fold_in(streams_of[6], 71), 0)
    owned_blocks = draw_owned_blocks(jax.random.fold_in(streams_of[6], 71), 0)
    occ_coef = scatter_about(streams_of[4], (NBLK, OCC, BLK), BLK ** -0.5, 0.5, ((0, 8),))
    vir_coef = scatter_about(streams_of[5], (NAO, V), (BLK * ALL_SLOTS // 2) ** -0.5, 0.109375, ((0, 8), (1, 4)))
    return {"blocks": blocks, "pairs": pairs, "counts": counts, "owned_blocks": owned_blocks, "occ_coef": occ_coef, "vir_coef": vir_coef}


def half_slab(args):
    block, coef, in_use = args
    value = jnp.einsum("im,pmn->pin", coef.astype(jnp.float32), block.astype(jnp.float32))
    return jnp.where(in_use, value, jnp.zeros_like(value)).astype(jnp.bfloat16)


def reference(blocks, pairs, counts, owned_blocks, occ_coef, vir_coef):
    total_blocks = owned_blocks.shape[0]
    slot_total = pairs.shape[0]
    slot_count = slot_total // N_AO
    block_width = blocks.shape[2]
    positions = jnp.arange(total_blocks, dtype=jnp.int32)
    place = jnp.zeros((total_blocks,), jnp.int32).at[owned_blocks].set(positions)
    in_use = (jnp.arange(slot_count, dtype=jnp.int32)[None, :] < counts[:, None]).reshape(-1)
    row_first = place[pairs[:, 0]]
    row_second = place[pairs[:, 1]]
    slabs = lax.map(half_slab, (blocks, occ_coef[row_first], in_use))
    gathered = jax.ops.segment_sum(slabs.astype(jnp.float32), row_second, num_segments=total_blocks)
    gathered = gathered.astype(jnp.bfloat16)
    per_owner = total_blocks // N_AO
    occupied = occ_coef.shape[1]
    total = jnp.zeros((PS * occupied, vir_coef.shape[1]), jnp.float32)
    for owner_idx in range(N_AO):
        part = gathered[owner_idx * per_owner:(owner_idx + 1) * per_owner]
        left = jnp.transpose(part, (1, 2, 0, 3)).reshape(PS * occupied, per_owner * block_width)
        right = vir_coef[owner_idx * per_owner * block_width:(owner_idx + 1) * per_owner * block_width]
        term = jnp.dot(left, right, preferred_element_type=jnp.float32).astype(jnp.bfloat16)
        total = total + term.astype(jnp.float32)
    return total.reshape(PS, occupied, vir_coef.shape[1]).astype(jnp.bfloat16)
```

```python
import functools

import jax
import jax.numpy as jnp
from jax import lax
from jax.experimental import pallas as pl
from jax.experimental.pallas import tpu as pltpu
from jax.sharding import PartitionSpec as P

CHUNKS = 2


def block_place(block_ids, owned_all):
    hits = block_ids[..., None] == owned_all
    positions = jnp.arange(owned_all.shape[0], dtype=jnp.int32)
    return jnp.sum(jnp.where(hits, positions, 0), axis=-1)


def swap_ao(x, mask):
    size = lax.axis_size("ao")
    return lax.ppermute(x, "ao", [(i, i ^ mask) for i in range(size)])


def sum_kernel(dest_ref, *refs, pieces, width):
    out_ref, acc_ref = refs[-2], refs[-1]
    acc_ref[...] = jnp.zeros_like(acc_ref)
    for ref, start, count in zip(refs[:-2], *pieces):
        def add(t, carry, ref=ref, start=start):
            slot = dest_ref[start + t]

            @pl.when(slot >= 0)
            def _():
                acc_ref[slot] += ref[t].astype(jnp.float32)

            return carry

        lax.fori_loop(0, count, add, 0)
    for slot in range(acc_ref.shape[0]):
        out_ref[:, slot * width:(slot + 1) * width] = acc_ref[slot].astype(out_ref.dtype)


def sum_slots(arrays, dest, cap):
    rows, width = arrays[0].shape[1:]
    counts = [a.shape[0] for a in arrays]
    starts = [sum(counts[:i]) for i in range(len(counts))]
    vmem = pl.BlockSpec(memory_space=pltpu.VMEM)
    return pl.pallas_call(
        functools.partial(sum_kernel, pieces=(starts, counts), width=width),
        out_shape=jax.ShapeDtypeStruct((rows, cap * width), jnp.bfloat16),
        in_specs=[pl.BlockSpec(memory_space=pltpu.SMEM)] + [vmem] * len(arrays),
        out_specs=vmem,
        scratch_shapes=[pltpu.VMEM((cap, rows, width), jnp.float32)],
        cost_estimate=pl.CostEstimate(
            flops=2 * sum(counts) * rows * width * 8, transcendentals=0,
            bytes_accessed=2 * rows * width * (sum(counts) + cap)),
        name="sum_slots",
    )(dest, *arrays)


def pick_kernel(pick_ref, own_ref, other_ref, out_ref, *, per_owner):
    slot = pick_ref[pl.program_id(0)]

    @pl.when(slot < per_owner)
    def _():
        out_ref[...] = own_ref[...]

    @pl.when(slot >= per_owner)
    def _():
        out_ref[...] = other_ref[...]


def pick_blocks(own, other, pick, width):
    cap = pick.shape[0]
    rows, columns = own.shape
    per_owner = rows // width
    return pl.pallas_call(
        functools.partial(pick_kernel, per_owner=per_owner),
        out_shape=jax.ShapeDtypeStruct((cap * width, columns), own.dtype),
        grid_spec=pltpu.PrefetchScalarGridSpec(
            num_scalar_prefetch=1,
            grid=(cap,),
            in_specs=[
                pl.BlockSpec((width, columns), lambda i, p: (jnp.minimum(p[i], per_owner - 1), 0)),
                pl.BlockSpec((width, columns), lambda i, p: (jnp.maximum(p[i] - per_owner, 0), 0)),
            ],
            out_specs=pl.BlockSpec((width, columns), lambda i, p: (i, 0)),
        ),
        cost_estimate=pl.CostEstimate(
            flops=cap * width * columns * 8, transcendentals=0, bytes_accessed=4 * cap * width * columns),
        name="pick_blocks",
    )(pick, own, other)


def plane_reduce(parts, chip, bits, vir, rows):
    orders = [list(range(bits)), list(range(bits))[::-1]]
    half = rows // 2
    count = 1 << bits

    def lhs(rels_by_part):
        picked = [
            lax.dynamic_index_in_dim(parts, chip ^ rel, 0, keepdims=False)[q * half:(q + 1) * half]
            for q in range(2) for rel in rels_by_part[q]
        ]
        return jnp.concatenate(picked, axis=0)

    keep = [list(range(count)), list(range(count))]
    values = [dict(), dict()]
    received = [dict(), dict()]
    for step in range(bits):
        flag = [1 << orders[q][step] for q in range(2)]
        send = [[r for r in keep[q] if r & flag[q]] for q in range(2)]
        keep = [[r for r in keep[q] if not r & flag[q]] for q in range(2)]
        if step == 0:
            first = jnp.dot(lhs(send), vir, preferred_element_type=jnp.float32).astype(jnp.bfloat16)
            n = len(send[0]) * half
            out = [first[:n], first[n:]]
        else:
            out = [
                jnp.concatenate([values[q][r] for r in send[q]], axis=0).astype(jnp.bfloat16)
                for q in range(2)
            ]
        got = [swap_ao(out[q], flag[q] << 1) for q in range(2)]
        if step == 0:
            second = jnp.dot(lhs(keep), vir, preferred_element_type=jnp.float32)
            for q in range(2):
                for at, r in enumerate(keep[q]):
                    start = (q * len(keep[0]) + at) * half
                    values[q][r] = second[start:start + half]
        for q in range(2):
            for at, r in enumerate(keep[q]):
                values[q][r] = values[q][r] + got[q][at * half:(at + 1) * half].astype(jnp.float32)
    return [values[q][0].astype(jnp.bfloat16) for q in range(2)]


def per_device(blocks, pairs, counts, owned_blocks, occ_coef, vir_coef):
    groups = lax.axis_size("ao")
    depth = lax.axis_size("aux")
    me = lax.axis_index("ao")
    core = me % 2
    chip = me // 2
    chips = groups // 2
    bits = chips.bit_length() - 1
    slots = blocks.shape[0]
    aux_depth = blocks.shape[1]
    width = blocks.shape[3]
    occupied = occ_coef.shape[1]
    per_owner = owned_blocks.shape[0]
    total_blocks = per_owner * groups

    vir_other = swap_ao(vir_coef, 1)

    ints = jnp.concatenate([pairs.reshape(-1), counts, owned_blocks])[None, :]
    all_ints = lax.all_gather(ints, "ao", axis=0, tiled=True)
    occ_all = lax.all_gather(occ_coef, "ao", axis=0, tiled=True)
    all_pairs = all_ints[:, :2 * slots].reshape(groups, slots, 2)
    all_counts = all_ints[:, 2 * slots]
    all_owned = all_ints[:, 2 * slots + 1:].reshape(-1)

    slot_ids = jnp.arange(slots, dtype=jnp.int32)
    live = slot_ids[None, :] < all_counts[:, None]
    place = jnp.where(live, block_place(all_pairs[:, :, 1], all_owned), -1)
    positions = jnp.arange(total_blocks, dtype=jnp.int32)
    used = jnp.any(place[:, :, None] == positions, axis=(0, 1))
    fullest = jnp.max(jnp.sum(used.reshape(chips, 2 * per_owner).astype(jnp.int32), axis=1))

    local = jnp.arange(2 * per_owner, dtype=jnp.int32)
    local_pos = (me ^ (local // per_owner)) * per_owner + local % per_owner
    hit = place[:, :, None] == local_pos
    local_used = jnp.any(hit, axis=(0, 1))
    rank = jnp.sum((local[None, :] < local[:, None]) & local_used[None, :], axis=1).astype(jnp.int32)
    target = jnp.sum(jnp.where(hit, rank + 1, 0), axis=-1).astype(jnp.int32) - 1

    occ_pick = occ_all[block_place(pairs[:, 0], all_owned)]
    slab = jnp.einsum("sim,spmn->spin", occ_pick, blocks, preferred_element_type=jnp.float32)
    slab = jnp.where((slot_ids < counts[0])[:, None, None, None], slab, 0.0).astype(jnp.bfloat16)
    rows = aux_depth // 2 * occupied
    slab = slab.reshape(slots, 2, rows, width)
    mine = lax.dynamic_index_in_dim(slab, core, 1, keepdims=False)
    theirs = lax.dynamic_index_in_dim(slab, 1 - core, 1, keepdims=False)
    from_core = swap_ao(theirs, 1)
    step = rows // CHUNKS

    def rest(cap, mine, from_core, target, local_used, rank, vir_own, vir_other):
        order = jnp.arange(cap, dtype=jnp.int32)
        pick = jnp.sum(
            jnp.where((rank[None, :] == order[:, None]) & local_used[None, :], local[None, :], 0), axis=1)
        pick = jnp.where(order < jnp.sum(local_used.astype(jnp.int32)), pick, 2 * per_owner - 1).astype(jnp.int32)
        vir = pick_blocks(vir_own, vir_other, pick, width)

        def targets(rel, parts):
            rows_of = [target[2 * (chip ^ rel) + (core ^ part)] for part in parts]
            return jnp.concatenate(rows_of)

        outs = []
        for c in range(CHUNKS):
            own = jnp.concatenate(
                [mine[:, c * step:(c + 1) * step], from_core[:, c * step:(c + 1) * step]], axis=0)
            arrays, dests = [own], [targets(0, (0, 1))]
            single = {}
            for b in range(bits):
                single[1 << b] = swap_ao(own, 2 << b)
                arrays.append(single[1 << b])
                dests.append(targets(1 << b, (0, 1)))
            for q in range(2):
                done = {r: a[q * slots:(q + 1) * slots] for r, a in single.items()}
                order_of = range(bits) if q == 0 else range(bits)[::-1]
                for b in order_of:
                    for r in list(done):
                        if r < (1 << bits) and not r & (1 << b) and (r | (1 << b)) not in done:
                            if all(not r & (1 << o) or (b > o if q == 0 else b < o) for o in range(bits)):
                                done[r | (1 << b)] = swap_ao(done[r], 2 << b)
                                arrays.append(done[r | (1 << b)])
                                dests.append(targets(r | (1 << b), (q,)))
            summed = sum_slots(arrays, jnp.concatenate(dests), cap)
            gathered = lax.all_gather(summed, "aux", axis=0, tiled=False)
            outs += plane_reduce(gathered, chip, bits, vir, step)
        return jnp.concatenate(outs, axis=0)

    most = 2 * per_owner
    small = most * 3 // 5
    operands = (mine, from_core, target, local_used, rank, vir_coef, vir_other)
    result = lax.cond(
        fullest <= small, functools.partial(rest, small), functools.partial(rest, most), *operands)
    return result.reshape(aux_depth // 2, occupied, vir_coef.shape[1])


def solution(mesh):
    in_specs = (
        P("ao", "aux", None, None),
        P("ao", None),
        P("ao"),
        P("ao"),
        P("ao", None, None),
        P("ao", "aux"),
    )
    out_specs = P("ao", None, "aux")
    return jax.shard_map(
        per_device, mesh=mesh, in_specs=in_specs, out_specs=out_specs, check_vma=False
    )
```

```python
import functools

import jax
import jax.numpy as jnp
from jax import lax
from jax.experimental import pallas as pl
from jax.experimental.pallas import tpu as pltpu
from jax.sharding import PartitionSpec as P

CHUNKS = 2
COLUMN_TILE = 256
SMEM = pl.BlockSpec(memory_space=pltpu.SMEM)
VMEM = pl.BlockSpec(memory_space=pltpu.VMEM)
ANY = pl.BlockSpec(memory_space=pl.ANY)


def swap_ao(x, mask):
    size = lax.axis_size("ao")
    return lax.ppermute(x, "ao", [(i, i ^ mask) for i in range(size)])


def shift_aux(x, by, first, last):
    return lax.ppermute(x, "aux", [(i, i + by) for i in range(first, last)])


def loop(count, body):
    lax.fori_loop(0, count, lambda i, c: (body(i), c)[1], 0)


def plan_kernel(me_ref, ints_ref, occ_ref, dest_ref, pack_ref, pick_ref, load_ref, place, used, lmap, *,
                groups, slots, per_owner):
    me = me_ref[0]
    core, chip = me % 2, me // 2
    chips = groups // 2
    both = 2 * slots
    span = 2 * per_owner
    owned_at = both + 1

    def owned(k):
        place[ints_ref[k // per_owner, 0, owned_at + k % per_owner]] = k
        used[k] = 0

    loop(groups * per_owner, owned)

    def clear(k):
        load_ref[k] = 0

    loop(chips * chips + 1, clear)

    def occ(s):
        occ_ref[s] = place[ints_ref[me, 0, 2 * s]]

    loop(slots, occ)

    def scan(t):
        g, s = t // slots, t % slots
        live = (s < ints_ref[g, 0, both]).astype(jnp.int32)
        pos = place[ints_ref[g, 0, 2 * s + 1]]
        used[pos] = jnp.maximum(used[pos], live)
        at = (g // 2) * chips + pos // span
        load_ref[at] += live

    loop(groups * slots, scan)

    def heaviest(at, worst):
        return jnp.maximum(worst, jnp.where(at // chips == at % chips, 0, load_ref[at]))

    load_ref[chips * chips] = lax.fori_loop(0, chips * chips, heaviest, 0)

    def fullest(c, worst):
        total = lax.fori_loop(0, span, lambda k, n: n + used[c * span + k], 0)
        return jnp.maximum(worst, total)

    load_ref[chips * chips + 1] = lax.fori_loop(0, chips, fullest, 0)

    def clear_pick(k):
        pick_ref[k] = 0

    loop(span, clear_pick)

    def rank(k, n):
        pos = (me ^ (k // per_owner)) * per_owner + k % per_owner
        lmap[pos] = n
        pick_ref[n] = jnp.where(used[pos] > 0, k, pick_ref[n])
        return n + used[pos]

    lax.fori_loop(0, span, rank, 0)

    def slot_of(rel, t):
        g = 2 * (chip ^ rel) + (core ^ (t // slots))
        s = t % slots
        live = s < ints_ref[g, 0, both]
        return live, place[ints_ref[g, 0, 2 * s + 1]]

    def clear_dest(k):
        dest_ref[k] = -1
        pack_ref[k] = 0

    loop(chips * both, clear_dest)

    def own(t):
        live, pos = slot_of(0, t)
        keep = live & (pos // span == chip)
        dest_ref[t] = jnp.where(keep, lmap[pos], -1)

    loop(both, own)

    def other(rel, c):
        def incoming(t, n):
            live, pos = slot_of(rel, t)
            keep = live & (pos // span == chip)
            at = rel * both + n
            dest_ref[at] = jnp.where(keep, lmap[pos], -1)
            return n + keep.astype(jnp.int32)

        lax.fori_loop(0, both, incoming, 0)

        def outgoing(t, n):
            live, pos = slot_of(0, t)
            keep = live & (pos // span == chip ^ rel)
            at = rel * both + n
            pack_ref[at] = jnp.where(keep, t, pack_ref[at])
            return n + keep.astype(jnp.int32)

        lax.fori_loop(0, both, outgoing, 0)
        return c

    lax.fori_loop(1, chips, other, 0)


def make_plan(me, all_ints, groups, slots, per_owner):
    chips = groups // 2
    total = groups * per_owner
    i32 = lambda n: jax.ShapeDtypeStruct((n,), jnp.int32)
    return pl.pallas_call(
        functools.partial(plan_kernel, groups=groups, slots=slots, per_owner=per_owner),
        out_shape=(i32(slots), i32(chips * 2 * slots + 1), i32(chips * 2 * slots + 1),
                   i32(2 * per_owner + 1), i32(chips * chips + 2)),
        in_specs=[SMEM, SMEM],
        out_specs=(SMEM,) * 5,
        scratch_shapes=[pltpu.SMEM((total,), jnp.int32)] * 3,
        name="plan",
    )(me[None], all_ints)


def pack_kernel(pack_ref, mine_ref, theirs_ref, *out_refs, slots, both):
    for rel, out_ref in enumerate(out_refs, 1):
        def copy(i, out_ref=out_ref, rel=rel):
            t = pack_ref[rel * both + i]

            @pl.when(t < slots)
            def _():
                out_ref[i] = mine_ref[t]

            @pl.when(t >= slots)
            def _():
                out_ref[i] = theirs_ref[t - slots]

        loop(out_ref.shape[0], copy)


def pack_slots(mine, theirs, pack, chips, cap, row0, rows):
    slots, _, width = mine.shape
    spec = pl.BlockSpec((slots, rows, width), lambda i, p: (0, row0 // rows, 0))
    return pl.pallas_call(
        functools.partial(pack_kernel, slots=slots, both=2 * slots),
        out_shape=(jax.ShapeDtypeStruct((cap, rows, width), mine.dtype),) * (chips - 1),
        grid_spec=pltpu.PrefetchScalarGridSpec(
            num_scalar_prefetch=1, grid=(1,), in_specs=[spec, spec],
            out_specs=(pl.BlockSpec((cap, rows, width), lambda i, p: (0, 0, 0)),) * (chips - 1)),
        cost_estimate=pl.CostEstimate(
            flops=8 * cap * rows * width, transcendentals=0, bytes_accessed=8 * cap * rows * width),
        name="pack_slots",
    )(pack, mine, theirs)


def sum_kernel(dest_ref, *refs, starts, width):
    out_ref, acc_ref = refs[-2], refs[-1]
    acc_ref[...] = jnp.zeros_like(acc_ref)
    for ref, start in zip(refs[:-2], starts):
        def add(t, ref=ref, start=start):
            slot = dest_ref[start + t]

            @pl.when(slot >= 0)
            def _():
                acc_ref[slot] += ref[t].astype(jnp.float32)

        loop(ref.shape[0], add)
    for slot in range(acc_ref.shape[0]):
        out_ref[:, slot * width:(slot + 1) * width] = acc_ref[slot].astype(out_ref.dtype)


def sum_slots(mine, theirs, received, dest, blocks, row0, rows):
    slots, _, width = mine.shape
    spec = pl.BlockSpec((slots, rows, width), lambda i, p: (0, row0 // rows, 0))
    whole = pl.BlockSpec(received[0].shape, lambda i, p: (0, 0, 0))
    starts = [0, slots] + [2 * slots * rel for rel in range(1, len(received) + 1)]
    read = 2 * slots + len(received) * received[0].shape[0]
    return pl.pallas_call(
        functools.partial(sum_kernel, starts=starts, width=width),
        out_shape=jax.ShapeDtypeStruct((rows, blocks * width), jnp.bfloat16),
        grid_spec=pltpu.PrefetchScalarGridSpec(
            num_scalar_prefetch=1, grid=(1,), in_specs=[spec, spec] + [whole] * len(received),
            out_specs=pl.BlockSpec((rows, blocks * width), lambda i, p: (0, 0)),
            scratch_shapes=[pltpu.VMEM((blocks, rows, width), jnp.float32)]),
        cost_estimate=pl.CostEstimate(
            flops=8 * read * rows * width, transcendentals=0,
            bytes_accessed=2 * rows * width * (read + blocks)),
        name="sum_slots",
    )(dest, mine, theirs, *received)


def multiply_kernel(at_ref, pick_ref, *refs, depth, pieces, half, width, blocks, per_owner):
    sources = refs[:2 * depth - 1]
    own, other = refs[2 * depth - 1:2 * depth + 1]
    outs = refs[2 * depth + 1:2 * depth + 5]
    rows, coef, row_sem, coef_sem = refs[2 * depth + 5:]
    chip, mine = at_ref[0], at_ref[1]

    def row_copy(n, source):
        q, _ = pieces[n]
        return pltpu.make_async_copy(
            source.at[pl.ds(q * half, half)], rows.at[pl.ds(n * half, half)], row_sem.at[n])

    for n, (q, rel) in enumerate(pieces):
        from_here = mine - (chip ^ rel)
        for s, source in enumerate(sources):
            @pl.when(from_here == s - (depth - 1))
            def _(n=n, source=source):
                row_copy(n, source).start()

    def coef_copy(block, source, at):
        return pltpu.make_async_copy(
            source.at[pl.ds(at * width, width)], coef.at[pl.ds(block * width, width)], coef_sem.at[block])

    def start(block):
        at = pick_ref[block]

        @pl.when(at < per_owner)
        def _():
            coef_copy(block, own, at).start()

        @pl.when(at >= per_owner)
        def _():
            coef_copy(block, other, at - per_owner).start()

    loop(blocks, start)
    for n in range(len(pieces)):
        row_copy(n, sources[0]).wait()
    loop(blocks, lambda block: coef_copy(block, own, 0).wait())

    def tile(i):
        columns = pl.ds(pl.multiple_of(i * COLUMN_TILE, COLUMN_TILE), COLUMN_TILE)
        value = jnp.dot(rows[...], coef[:, columns], preferred_element_type=jnp.float32)
        size = value.shape[0] // 4
        for n, out in enumerate(outs):
            out[:, columns] = value[n * size:(n + 1) * size].astype(out.dtype)

    loop(coef.shape[1] // COLUMN_TILE, tile)


def multiply(at, pick, sources, own, other, pieces, blocks, width):
    depth = (len(sources) + 1) // 2
    rows, inner = sources[0].shape
    half = rows // 2
    columns = own.shape[1]
    quarter = len(pieces) * half // 4
    out = jax.ShapeDtypeStruct((quarter, columns), jnp.bfloat16)
    return pl.pallas_call(
        functools.partial(multiply_kernel, depth=depth, pieces=pieces, half=half, width=width,
                          blocks=blocks, per_owner=own.shape[0] // width),
        out_shape=(out,) * 4,
        in_specs=[SMEM, SMEM] + [ANY] * (len(sources) + 2),
        out_specs=(VMEM,) * 4,
        scratch_shapes=[
            pltpu.VMEM((len(pieces) * half, inner), jnp.bfloat16),
            pltpu.VMEM((blocks * width, columns), jnp.bfloat16),
            pltpu.SemaphoreType.DMA((len(pieces),)),
            pltpu.SemaphoreType.DMA((blocks,)),
        ],
        cost_estimate=pl.CostEstimate(
            flops=2 * len(pieces) * half * inner * columns, transcendentals=0,
            bytes_accessed=2 * (inner * columns + len(pieces) * half * (inner + columns))),
        name="multiply",
    )(at, pick, *sources, own, other)


def per_device(blocks, pairs, counts, owned_blocks, occ_coef, vir_coef):
    groups = lax.axis_size("ao")
    depth = lax.axis_size("aux")
    me = lax.axis_index("ao")
    layer = lax.axis_index("aux")
    core, chip = me % 2, me // 2
    chips = groups // 2
    bits = chips.bit_length() - 1
    slots, aux_depth, _, width = blocks.shape
    occupied = occ_coef.shape[1]
    per_owner = owned_blocks.shape[0]

    vir_other = swap_ao(vir_coef, 1)

    ints = jnp.concatenate([pairs.reshape(-1), counts, owned_blocks])
    ints = jnp.pad(ints, (0, -ints.shape[0] % 128))[None, None, :]
    all_ints = lax.all_gather(ints, "ao", axis=0, tiled=True)
    occ_all = lax.all_gather(occ_coef, "ao", axis=0, tiled=True)
    occ_at, dest, pack, pick, load = make_plan(me, all_ints, groups, slots, per_owner)

    slab = jnp.einsum("sim,spmn->spin", occ_all[occ_at], blocks, preferred_element_type=jnp.float32)
    in_use = jnp.arange(slots, dtype=jnp.int32) < counts[0]
    slab = jnp.where(in_use[:, None, None, None], slab, 0.0).astype(jnp.bfloat16)
    rows = aux_depth // 2 * occupied
    slab = slab.reshape(slots, 2, rows, width)
    mine = lax.dynamic_index_in_dim(slab, core, 1, keepdims=False)
    theirs = swap_ao(lax.dynamic_index_in_dim(slab, 1 - core, 1, keepdims=False), 1)
    step = rows // CHUNKS
    half = step // 2
    at = jnp.stack([chip, layer]).astype(jnp.int32)

    orders = [list(range(bits)), list(range(bits))[::-1]]
    flags = [[1 << b for b in order] for order in orders]
    send = [[r for r in range(chips) if r & flags[q][0]] for q in range(2)]
    keep = [[r for r in range(chips) if not r & flags[q][0]] for q in range(2)]
    pieces = [(q, r) for part in (send, keep) for q in range(2) for r in part[q]]

    def rest(cap, used_blocks, mine, theirs, dest, pack, pick, vir_own, vir_other):
        gathered = []
        for c in range(CHUNKS):
            outgoing = pack_slots(mine, theirs, pack, chips, cap, c * step, step)
            received = [swap_ao(x, 2 * rel) for rel, x in enumerate(outgoing, 1)]
            own = sum_slots(mine, theirs, received, dest, used_blocks, c * step, step)
            lower, upper = [], []
            up = down = own
            for hop in range(depth - 1):
                up = shift_aux(up, 1, hop, depth - 1)
                down = shift_aux(down, -1, 1, depth - hop)
                lower.append(up)
                upper.append(down)
            gathered.append(upper[::-1] + [own] + lower)

        outs = []
        for c in range(CHUNKS):
            product = multiply(at, pick, gathered[c], vir_own, vir_other, pieces, used_blocks, width)
            out, held = product[:2], product[2:]
            held_rels = keep
            held = [{r: held[q][n * half:(n + 1) * half] for n, r in enumerate(keep[q])} for q in range(2)]
            for b in range(bits):
                got = [swap_ao(out[q], 2 * flags[q][b]) for q in range(2)]
                total = [
                    {r: held[q][r].astype(jnp.float32) + got[q][n * half:(n + 1) * half].astype(jnp.float32)
                     for n, r in enumerate(sorted(held[q]))}
                    for q in range(2)
                ]
                if b + 1 < bits:
                    flag = [flags[q][b + 1] for q in range(2)]
                    out = [
                        jnp.concatenate([total[q][r] for r in sorted(total[q]) if r & flag[q]]).astype(jnp.bfloat16)
                        for q in range(2)
                    ]
                    held = [{r: v for r, v in total[q].items() if not r & flag[q]} for q in range(2)]
            outs += [total[q][0].astype(jnp.bfloat16) for q in range(2)]
        return jnp.concatenate(outs, axis=0)

    most = 2 * per_owner
    few = most * 3 // 5
    fits = (load[chips * chips] <= slots) & (load[chips * chips + 1] <= few)
    result = lax.cond(
        fits, functools.partial(rest, slots, few), functools.partial(rest, 2 * slots, most),
        mine, theirs, dest, pack, pick, vir_coef, vir_other)
    return result.reshape(aux_depth // 2, occupied, vir_coef.shape[1])


def solution(mesh):
    in_specs = (
        P("ao", "aux", None, None),
        P("ao", None),
        P("ao"),
        P("ao"),
        P("ao", None, None),
        P("ao", "aux"),
    )
    out_specs = P("ao", None, "aux")
    return jax.shard_map(
        per_device, mesh=mesh, in_specs=in_specs, out_specs=out_specs, check_vma=False
    )
```

```python
import functools

import jax
import jax.numpy as jnp
from jax import lax
from jax.experimental import pallas as pl
from jax.experimental.pallas import tpu as pltpu
from jax.sharding import PartitionSpec as P

CHUNKS = 2
COLUMN_TILE = 256
SMEM = pl.BlockSpec(memory_space=pltpu.SMEM)
VMEM = pl.BlockSpec(memory_space=pltpu.VMEM)
ANY = pl.BlockSpec(memory_space=pl.ANY)


def swap_ao(x, mask):
    size = lax.axis_size("ao")
    return lax.ppermute(x, "ao", [(i, i ^ mask) for i in range(size)])


def shift_aux(x, by, first, last):
    return lax.ppermute(x, "aux", [(i, i + by) for i in range(first, last)])


def loop(count, body):
    lax.fori_loop(0, count, lambda i, c: (body(i), c)[1], 0)


def room(*arrays):
    return sum(a.size * a.dtype.itemsize for a in arrays) + (4 << 20)


def plan_kernel(me_ref, ints_ref, occ_ref, dest_ref, pack_ref, pick_ref, load_ref, place, used, lmap, info, *,
                groups, slots, per_owner):
    me = me_ref[0]
    core, chip = me % 2, me // 2
    chips = groups // 2
    both = 2 * slots
    span = 2 * per_owner
    total = groups * per_owner
    shift = total.bit_length()

    for k in range(total):
        place[ints_ref[k // per_owner, 0, both + 1 + k % per_owner]] = k + ((k // span) << shift)
        used[k] = 0
    for k in range(chips * chips):
        load_ref[k] = 0
    for s in range(slots):
        occ_ref[s] = place[ints_ref[me, 0, 2 * s]] & ((1 << shift) - 1)
    for g in range(groups):
        count = ints_ref[g, 0, both]
        for s in range(slots):
            live = s < count
            where = place[ints_ref[g, 0, 2 * s + 1]]
            info[g * slots + s] = jnp.where(live, where, -1)
            pos = where & ((1 << shift) - 1)
            used[pos] = jnp.where(live, 1, used[pos])
            at = (g // 2) * chips + (where >> shift)
            load_ref[at] = load_ref[at] + live.astype(jnp.int32)

    sent = blocks = jnp.int32(0)
    for c in range(chips):
        for d in range(chips):
            if c != d:
                sent = jnp.maximum(sent, load_ref[c * chips + d])
        filled = jnp.int32(0)
        for k in range(span):
            filled = filled + used[c * span + k]
        blocks = jnp.maximum(blocks, filled)
    load_ref[chips * chips] = sent
    load_ref[chips * chips + 1] = blocks

    for k in range(span):
        pick_ref[k] = 0
    n = jnp.int32(0)
    for h in range(2):
        base = (me ^ h) * per_owner
        for k in range(per_owner):
            lmap[base + k] = n
            flag = used[base + k]
            pick_ref[n] = jnp.where(flag > 0, h * per_owner + k, pick_ref[n])
            n = n + flag

    for k in range(chips * both):
        dest_ref[k] = -1
        pack_ref[k] = 0
    for rel in range(chips):
        incoming = outgoing = jnp.int32(rel * both)
        for h in range(2):
            from_base = (2 * (chip ^ rel) + (core ^ h)) * slots
            own_base = (2 * chip + (core ^ h)) * slots
            for s in range(slots):
                there = info[from_base + s]
                keep = (there >> shift) == chip
                slot = jnp.where(keep, lmap[jnp.maximum(there, 0) & ((1 << shift) - 1)], -1)
                if rel == 0:
                    dest_ref[h * slots + s] = slot
                else:
                    dest_ref[incoming] = slot
                    incoming = incoming + keep.astype(jnp.int32)
                    leave = (info[own_base + s] >> shift) == (chip ^ rel)
                    pack_ref[outgoing] = jnp.where(leave, h * slots + s, pack_ref[outgoing])
                    outgoing = outgoing + leave.astype(jnp.int32)


def make_plan(me, all_ints, groups, slots, per_owner):
    chips = groups // 2
    total = groups * per_owner
    i32 = lambda n: jax.ShapeDtypeStruct((n,), jnp.int32)
    return pl.pallas_call(
        functools.partial(plan_kernel, groups=groups, slots=slots, per_owner=per_owner),
        out_shape=(i32(slots), i32(chips * 2 * slots + 1), i32(chips * 2 * slots + 1),
                   i32(2 * per_owner + 1), i32(chips * chips + 2)),
        in_specs=[SMEM, SMEM],
        out_specs=(SMEM,) * 5,
        scratch_shapes=[pltpu.SMEM((total,), jnp.int32)] * 3 + [pltpu.SMEM((groups * slots,), jnp.int32)],
        compiler_params=pltpu.CompilerParams(vmem_limit_bytes=1 << 20),
        name="plan",
    )(me[None], all_ints)


def pack_kernel(pack_ref, mine_ref, theirs_ref, *out_refs, slots, both, chips):
    for n, out_ref in enumerate(out_refs):
        c, rel = n // (chips - 1), n % (chips - 1) + 1
        rows = pl.ds(c * out_ref.shape[1], out_ref.shape[1])

        def copy(i, out_ref=out_ref, rel=rel, rows=rows):
            t = pack_ref[rel * both + i]

            @pl.when(t < slots)
            def _():
                out_ref[i] = mine_ref[t, rows]

            @pl.when(t >= slots)
            def _():
                out_ref[i] = theirs_ref[t - slots, rows]

        loop(out_ref.shape[0], copy)


def pack_slots(mine, theirs, pack, chips, cap):
    slots, rows, width = mine.shape
    out = jax.ShapeDtypeStruct((cap, rows // CHUNKS, width), mine.dtype)
    outs = (out,) * ((chips - 1) * CHUNKS)
    return pl.pallas_call(
        functools.partial(pack_kernel, slots=slots, both=2 * slots, chips=chips),
        out_shape=outs,
        in_specs=[SMEM, VMEM, VMEM],
        out_specs=(VMEM,) * len(outs),
        compiler_params=pltpu.CompilerParams(vmem_limit_bytes=room(mine, theirs, *outs)),
        cost_estimate=pl.CostEstimate(
            flops=8 * cap * rows * width, transcendentals=0, bytes_accessed=8 * cap * rows * width),
        name="pack_slots",
    )(pack, mine, theirs)


def sum_kernel(dest_ref, mine_ref, theirs_ref, *refs, starts, width, row0):
    received, out_ref, acc_ref = refs[:-2], refs[-2], refs[-1]
    rows = out_ref.shape[0]
    acc_ref[...] = jnp.zeros_like(acc_ref)
    for n, start in enumerate(starts):
        ref = mine_ref if n == 0 else theirs_ref if n == 1 else received[n - 2]
        first = row0 if n < 2 else 0

        def add(t, ref=ref, start=start, first=first):
            slot = dest_ref[start + t]

            @pl.when(slot >= 0)
            def _():
                acc_ref[slot] += ref[t, first:first + rows].astype(jnp.float32)

        loop(ref.shape[0], add)
    for slot in range(acc_ref.shape[0]):
        out_ref[:, slot * width:(slot + 1) * width] = acc_ref[slot].astype(out_ref.dtype)


def sum_slots(mine, theirs, received, dest, blocks, row0):
    slots, _, width = mine.shape
    rows = received[0].shape[1]
    starts = [0, slots] + [2 * slots * rel for rel in range(1, len(received) + 1)]
    read = 2 * slots + len(received) * received[0].shape[0]
    out = jax.ShapeDtypeStruct((rows, blocks * width), jnp.bfloat16)
    return pl.pallas_call(
        functools.partial(sum_kernel, starts=starts, width=width, row0=row0),
        out_shape=out,
        in_specs=[SMEM] + [VMEM] * (2 + len(received)),
        out_specs=VMEM,
        scratch_shapes=[pltpu.VMEM((blocks, rows, width), jnp.float32)],
        compiler_params=pltpu.CompilerParams(vmem_limit_bytes=room(mine, theirs, *received, out, out, out)),
        cost_estimate=pl.CostEstimate(
            flops=8 * read * rows * width, transcendentals=0,
            bytes_accessed=2 * rows * width * (read + blocks)),
        name="sum_slots",
    )(dest, mine, theirs, *received)


def pick_kernel(pick_ref, own, other, out_ref, sem, *, width, blocks, per_owner):
    def copy(block, source, at):
        return pltpu.make_async_copy(
            source.at[pl.ds(at * width, width)], out_ref.at[pl.ds(block * width, width)], sem.at[block])

    def start(block):
        at = pick_ref[block]

        @pl.when(at < per_owner)
        def _():
            copy(block, own, at).start()

        @pl.when(at >= per_owner)
        def _():
            copy(block, other, at - per_owner).start()

    loop(blocks, start)
    loop(blocks, lambda block: copy(block, own, 0).wait())


def pick_blocks(own, other, pick, blocks, width):
    out = jax.ShapeDtypeStruct((blocks * width, own.shape[1]), own.dtype)
    return pl.pallas_call(
        functools.partial(pick_kernel, width=width, blocks=blocks, per_owner=own.shape[0] // width),
        out_shape=out,
        in_specs=[SMEM, ANY, ANY],
        out_specs=VMEM,
        scratch_shapes=[pltpu.SemaphoreType.DMA((blocks,))],
        compiler_params=pltpu.CompilerParams(vmem_limit_bytes=room(out)),
        cost_estimate=pl.CostEstimate(
            flops=8 * out.size, transcendentals=0, bytes_accessed=2 * out.size),
        name="pick_blocks",
    )(pick, own, other)


def multiply_kernel(at_ref, *refs, depth, pieces, half):
    sources = refs[:2 * depth - 1]
    coef = refs[2 * depth - 1]
    outs = refs[2 * depth:2 * depth + 4]
    rows, row_sem = refs[2 * depth + 4:]
    chip, mine = at_ref[0], at_ref[1]

    def row_copy(n, source):
        return pltpu.make_async_copy(
            source.at[pl.ds(pieces[n][0] * half, half)], rows.at[pl.ds(n * half, half)], row_sem.at[n])

    for n, (q, rel) in enumerate(pieces):
        from_here = mine - (chip ^ rel)
        for s, source in enumerate(sources):
            @pl.when(from_here == s - (depth - 1))
            def _(n=n, source=source):
                row_copy(n, source).start()

    for n in range(len(pieces)):
        row_copy(n, sources[0]).wait()

    def tile(i):
        columns = pl.ds(pl.multiple_of(i * COLUMN_TILE, COLUMN_TILE), COLUMN_TILE)
        value = jnp.dot(rows[...], coef[:, columns], preferred_element_type=jnp.float32)
        size = value.shape[0] // 4
        for n, out in enumerate(outs):
            out[:, columns] = value[n * size:(n + 1) * size].astype(out.dtype)

    loop(coef.shape[1] // COLUMN_TILE, tile)


def multiply(at, sources, coef, pieces):
    depth = (len(sources) + 1) // 2
    rows, inner = sources[0].shape
    half = rows // 2
    columns = coef.shape[1]
    quarter = len(pieces) * half // 4
    out = jax.ShapeDtypeStruct((quarter, columns), jnp.bfloat16)
    taken = jax.ShapeDtypeStruct((len(pieces) * half, inner), jnp.bfloat16)
    return pl.pallas_call(
        functools.partial(multiply_kernel, depth=depth, pieces=pieces, half=half),
        out_shape=(out,) * 4,
        in_specs=[SMEM] + [ANY] * len(sources) + [VMEM],
        out_specs=(VMEM,) * 4,
        scratch_shapes=[pltpu.VMEM(taken.shape, taken.dtype), pltpu.SemaphoreType.DMA((len(pieces),))],
        compiler_params=pltpu.CompilerParams(vmem_limit_bytes=room(coef, taken, out, out, out, out)),
        cost_estimate=pl.CostEstimate(
            flops=2 * taken.size * columns, transcendentals=0,
            bytes_accessed=2 * (inner * columns + taken.size + 4 * out.size)),
        name="multiply",
    )(at, *sources, coef)


def per_device(blocks, pairs, counts, owned_blocks, occ_coef, vir_coef):
    groups = lax.axis_size("ao")
    depth = lax.axis_size("aux")
    me = lax.axis_index("ao")
    layer = lax.axis_index("aux")
    core, chip = me % 2, me // 2
    chips = groups // 2
    bits = chips.bit_length() - 1
    slots, aux_depth, _, width = blocks.shape
    occupied = occ_coef.shape[1]
    per_owner = owned_blocks.shape[0]

    vir_other = swap_ao(vir_coef, 1)

    ints = jnp.concatenate([pairs.reshape(-1), counts, owned_blocks])
    ints = jnp.pad(ints, (0, -ints.shape[0] % 128))[None, None, :]
    all_ints = lax.all_gather(ints, "ao", axis=0, tiled=True)
    occ_all = lax.all_gather(occ_coef, "ao", axis=0, tiled=True)
    occ_at, dest, pack, pick, load = make_plan(me, all_ints, groups, slots, per_owner)

    slab = jnp.einsum("sim,spmn->spin", occ_all[occ_at], blocks, preferred_element_type=jnp.float32)
    in_use = jnp.arange(slots, dtype=jnp.int32) < counts[0]
    slab = jnp.where(in_use[:, None, None, None], slab, 0.0).astype(jnp.bfloat16)
    rows = aux_depth // 2 * occupied
    slab = slab.reshape(slots, 2, rows, width)
    mine = lax.dynamic_index_in_dim(slab, core, 1, keepdims=False)
    theirs = swap_ao(lax.dynamic_index_in_dim(slab, 1 - core, 1, keepdims=False), 1)
    step = rows // CHUNKS
    half = step // 2
    at = jnp.stack([chip, layer]).astype(jnp.int32)

    orders = [list(range(bits)), list(range(bits))[::-1]]
    flags = [[1 << b for b in order] for order in orders]
    send = [[r for r in range(chips) if r & flags[q][0]] for q in range(2)]
    keep = [[r for r in range(chips) if not r & flags[q][0]] for q in range(2)]
    pieces = [(q, r) for part in (send, keep) for q in range(2) for r in part[q]]

    def rest(cap, used_blocks, mine, theirs, dest, pack, pick, vir_own, vir_other):
        outgoing = pack_slots(mine, theirs, pack, chips, cap)
        coef = pick_blocks(vir_own, vir_other, pick, used_blocks, width)
        gathered = []
        for c in range(CHUNKS):
            part = outgoing[c * (chips - 1):(c + 1) * (chips - 1)]
            received = [swap_ao(x, 2 * rel) for rel, x in enumerate(part, 1)]
            own = sum_slots(mine, theirs, received, dest, used_blocks, c * step)
            lower, upper = [], []
            for hop in range(1, depth):
                if hop < 3:
                    lower.append(shift_aux(own, hop, 0, depth - hop))
                    upper.append(shift_aux(own, -hop, hop, depth))
                else:
                    lower.append(shift_aux(lower[-1], 1, hop - 1, depth - 1))
                    upper.append(shift_aux(upper[-1], -1, 1, depth - hop + 1))
            gathered.append(upper[::-1] + [own] + lower)

        outs = []
        for c in range(CHUNKS):
            product = multiply(at, gathered[c], coef, pieces)
            out, held = product[:2], product[2:]
            held = [{r: held[q][n * half:(n + 1) * half] for n, r in enumerate(keep[q])} for q in range(2)]
            for b in range(bits):
                got = [swap_ao(out[q], 2 * flags[q][b]) for q in range(2)]
                total = [
                    {r: held[q][r].astype(jnp.float32) + got[q][n * half:(n + 1) * half].astype(jnp.float32)
                     for n, r in enumerate(sorted(held[q]))}
                    for q in range(2)
                ]
                if b + 1 < bits:
                    flag = [flags[q][b + 1] for q in range(2)]
                    out = [
                        jnp.concatenate([total[q][r] for r in sorted(total[q]) if r & flag[q]]).astype(jnp.bfloat16)
                        for q in range(2)
                    ]
                    held = [{r: v for r, v in total[q].items() if not r & flag[q]} for q in range(2)]
            outs += [total[q][0].astype(jnp.bfloat16) for q in range(2)]
        return jnp.concatenate(outs, axis=0)

    most = 2 * per_owner
    few = most * 3 // 5
    fits = (load[chips * chips] <= slots) & (load[chips * chips + 1] <= few)
    result = lax.cond(
        fits, functools.partial(rest, slots, few), functools.partial(rest, 2 * slots, most),
        mine, theirs, dest, pack, pick, vir_coef, vir_other)
    return result.reshape(aux_depth // 2, occupied, vir_coef.shape[1])


def solution(mesh):
    in_specs = (
        P("ao", "aux", None, None),
        P("ao", None),
        P("ao"),
        P("ao"),
        P("ao", None, None),
        P("ao", "aux"),
    )
    out_specs = P("ao", None, "aux")
    return jax.shard_map(
        per_device, mesh=mesh, in_specs=in_specs, out_specs=out_specs, check_vma=False
    )
```

```python
import functools

import jax
import jax.numpy as jnp
from jax import lax
from jax.experimental import pallas as pl
from jax.experimental.pallas import tpu as pltpu
from jax.sharding import PartitionSpec as P


GROUPS = ((1,), (1, 1, 1))
QUARTERS = 4
COLUMN_TILE = 768
SMEM = pl.BlockSpec(memory_space=pltpu.SMEM)
VMEM = pl.BlockSpec(memory_space=pltpu.VMEM)
ANY = pl.BlockSpec(memory_space=pl.ANY)


def swap_ao(x, mask):
    size = lax.axis_size("ao")
    return lax.ppermute(x, "ao", [(i, i ^ mask) for i in range(size)])


def swap_aux(x, mask):
    size = lax.axis_size("aux")
    return lax.ppermute(x, "aux", [(i, i ^ mask) for i in range(size)])


def loop(count, body):
    lax.fori_loop(0, count, lambda i, c: (body(i), c)[1], 0)


def room(*arrays):
    return sum(a.size * a.dtype.itemsize for a in arrays) + (4 << 20)


def plan_kernel(me_ref, ints_ref, occ_ref, dest_ref, pack_ref, pick_ref, load_ref, place, used, lmap, info, *,
                groups, slots, per_owner):
    me = me_ref[0]
    core, chip = me % 2, me // 2
    chips = groups // 2
    both = 2 * slots
    span = 2 * per_owner
    total = groups * per_owner
    shift = total.bit_length()

    for k in range(total):
        place[ints_ref[k // per_owner, 0, both + 1 + k % per_owner]] = k + ((k // span) << shift)
        used[k] = 0
    for k in range(chips * chips):
        load_ref[k] = 0
    for s in range(slots):
        occ_ref[s] = place[ints_ref[me, 0, 2 * s]] & ((1 << shift) - 1)
    for g in range(groups):
        count = ints_ref[g, 0, both]
        for s in range(slots):
            live = s < count
            where = place[ints_ref[g, 0, 2 * s + 1]]
            info[g * slots + s] = jnp.where(live, where, -1)
            pos = where & ((1 << shift) - 1)
            used[pos] = jnp.where(live, 1, used[pos])
            at = (g // 2) * chips + (where >> shift)
            load_ref[at] = load_ref[at] + live.astype(jnp.int32)

    sent = blocks = jnp.int32(0)
    for c in range(chips):
        for d in range(chips):
            if c != d:
                sent = jnp.maximum(sent, load_ref[c * chips + d])
        filled = jnp.int32(0)
        for k in range(span):
            filled = filled + used[c * span + k]
        blocks = jnp.maximum(blocks, filled)
    load_ref[chips * chips] = sent
    load_ref[chips * chips + 1] = blocks

    for k in range(span):
        pick_ref[k] = 0
    n = jnp.int32(0)
    for h in range(2):
        base = (me ^ h) * per_owner
        for k in range(per_owner):
            lmap[base + k] = n
            flag = used[base + k]
            pick_ref[n] = jnp.where(flag > 0, h * per_owner + k, pick_ref[n])
            n = n + flag

    for k in range(chips * both):
        dest_ref[k] = -1
        pack_ref[k] = 0
    for rel in range(chips):
        incoming = outgoing = jnp.int32(rel * both)
        for h in range(2):
            from_base = (2 * (chip ^ rel) + (core ^ h)) * slots
            own_base = (2 * chip + (core ^ h)) * slots
            for s in range(slots):
                there = info[from_base + s]
                keep = (there >> shift) == chip
                slot = jnp.where(keep, lmap[jnp.maximum(there, 0) & ((1 << shift) - 1)], -1)
                if rel == 0:
                    dest_ref[h * slots + s] = slot
                else:
                    dest_ref[incoming] = slot
                    incoming = incoming + keep.astype(jnp.int32)
                    leave = (info[own_base + s] >> shift) == (chip ^ rel)
                    pack_ref[outgoing] = jnp.where(leave, h * slots + s, pack_ref[outgoing])
                    outgoing = outgoing + leave.astype(jnp.int32)


def make_plan(me, all_ints, groups, slots, per_owner):
    chips = groups // 2
    total = groups * per_owner
    i32 = lambda n: jax.ShapeDtypeStruct((n,), jnp.int32)
    return pl.pallas_call(
        functools.partial(plan_kernel, groups=groups, slots=slots, per_owner=per_owner),
        out_shape=(i32(slots), i32(chips * 2 * slots + 1), i32(chips * 2 * slots + 1),
                   i32(2 * per_owner + 1), i32(chips * chips + 2)),
        in_specs=[SMEM, SMEM],
        out_specs=(SMEM,) * 5,
        scratch_shapes=[pltpu.SMEM((total,), jnp.int32)] * 3 + [pltpu.SMEM((groups * slots,), jnp.int32)],
        compiler_params=pltpu.CompilerParams(vmem_limit_bytes=1 << 20),
        name="plan",
    )(me[None], all_ints)


def pack_kernel(pack_ref, mine_ref, theirs_ref, *out_refs, slots, both, chips):
    row0 = 0
    for n, out_ref in enumerate(out_refs):
        rel = n % (chips - 1) + 1
        rows = pl.ds(row0, out_ref.shape[1])
        if rel == chips - 1:
            row0 += out_ref.shape[1]

        def copy(i, out_ref=out_ref, rel=rel, rows=rows):
            t = pack_ref[rel * both + i]

            @pl.when(t < slots)
            def _():
                out_ref[i] = mine_ref[t, rows]

            @pl.when(t >= slots)
            def _():
                out_ref[i] = theirs_ref[t - slots, rows]

        loop(out_ref.shape[0], copy)


def pack_slots(mine, theirs, pack, chips, cap):
    slots, rows, width = mine.shape
    outs = [
        jax.ShapeDtypeStruct((cap, sum(group) * rows // QUARTERS, width), mine.dtype)
        for group in GROUPS for _ in range(chips - 1)
    ]
    return pl.pallas_call(
        functools.partial(pack_kernel, slots=slots, both=2 * slots, chips=chips),
        out_shape=tuple(outs),
        in_specs=[SMEM, VMEM, VMEM],
        out_specs=(VMEM,) * len(outs),
        compiler_params=pltpu.CompilerParams(vmem_limit_bytes=room(mine, theirs, *outs)),
        cost_estimate=pl.CostEstimate(
            flops=8 * cap * rows * width, transcendentals=0, bytes_accessed=8 * cap * rows * width),
        name="pack_slots",
    )(pack, mine, theirs)


def sum_kernel(dest_ref, mine_ref, theirs_ref, *refs, starts, width, row0):
    received, outs, acc_ref = refs[:len(starts) - 2], refs[len(starts) - 2:-1], refs[-1]
    rows = acc_ref.shape[1]
    acc_ref[...] = jnp.zeros_like(acc_ref)
    for n, start in enumerate(starts):
        ref = mine_ref if n == 0 else theirs_ref if n == 1 else received[n - 2]
        first = row0 if n < 2 else 0

        def add(t, ref=ref, start=start, first=first):
            slot = dest_ref[start + t]

            @pl.when(slot >= 0)
            def _():
                acc_ref[slot] += ref[t, first:first + rows].astype(jnp.float32)

        loop(ref.shape[0], add)
    first = 0
    for out in outs:
        count = out.shape[0]
        for slot in range(acc_ref.shape[0]):
            out[:, slot * width:(slot + 1) * width] = acc_ref[slot, first:first + count].astype(out.dtype)
        first += count


def sum_slots(mine, theirs, received, dest, blocks, row0, sizes):
    slots, _, width = mine.shape
    rows = received[0].shape[1]
    starts = [0, slots] + [2 * slots * rel for rel in range(1, len(received) + 1)]
    read = 2 * slots + len(received) * received[0].shape[0]
    outs = [jax.ShapeDtypeStruct((size, blocks * width), jnp.bfloat16) for size in sizes]
    return pl.pallas_call(
        functools.partial(sum_kernel, starts=starts, width=width, row0=row0),
        out_shape=tuple(outs),
        in_specs=[SMEM] + [VMEM] * (2 + len(received)),
        out_specs=(VMEM,) * len(outs),
        scratch_shapes=[pltpu.VMEM((blocks, rows, width), jnp.float32)],
        compiler_params=pltpu.CompilerParams(vmem_limit_bytes=room(mine, theirs, *received, *outs, *outs, *outs)),
        cost_estimate=pl.CostEstimate(
            flops=8 * read * rows * width, transcendentals=0,
            bytes_accessed=2 * rows * width * (read + blocks)),
        name="sum_slots",
    )(dest, mine, theirs, *received)


def pick_kernel(pick_ref, own, other, out_ref, sem, *, width, blocks, per_owner):
    def copy(block, source, at):
        return pltpu.make_async_copy(
            source.at[pl.ds(at * width, width)], out_ref.at[pl.ds(block * width, width)], sem.at[block])

    def start(block):
        at = pick_ref[block]

        @pl.when(at < per_owner)
        def _():
            copy(block, own, at).start()

        @pl.when(at >= per_owner)
        def _():
            copy(block, other, at - per_owner).start()

    loop(blocks, start)
    loop(blocks, lambda block: copy(block, own, 0).wait())


def pick_blocks(own, other, pick, blocks, width):
    out = jax.ShapeDtypeStruct((blocks * width, own.shape[1]), own.dtype)
    return pl.pallas_call(
        functools.partial(pick_kernel, width=width, blocks=blocks, per_owner=own.shape[0] // width),
        out_shape=out,
        in_specs=[SMEM, ANY, ANY],
        out_specs=VMEM,
        scratch_shapes=[pltpu.SemaphoreType.DMA((blocks,))],
        compiler_params=pltpu.CompilerParams(vmem_limit_bytes=room(out)),
        cost_estimate=pl.CostEstimate(
            flops=8 * out.size, transcendentals=0, bytes_accessed=2 * out.size),
        name="pick_blocks",
    )(pick, own, other)


def multiply_kernel(at_ref, *refs, depth, pieces, half):
    sources, coef = refs[:depth], refs[depth]
    outs = refs[depth + 1:depth + 5]
    rows, row_sem = refs[depth + 5:]
    chip, mine = at_ref[0], at_ref[1]

    def row_copy(n, source):
        return pltpu.make_async_copy(
            source.at[pl.ds(pieces[n][0] * half, half)], rows.at[pl.ds(n * half, half)], row_sem.at[n])

    for n, (q, rel) in enumerate(pieces):
        apart = mine ^ chip ^ rel
        for s, source in enumerate(sources):
            @pl.when(apart == s)
            def _(n=n, source=source):
                row_copy(n, source).start()

    for n in range(len(pieces)):
        row_copy(n, sources[0]).wait()

    def tile(i):
        columns = pl.ds(pl.multiple_of(i * COLUMN_TILE, COLUMN_TILE), COLUMN_TILE)
        value = jnp.dot(rows[...], coef[:, columns], preferred_element_type=jnp.float32)
        size = value.shape[0] // 4
        for n, out in enumerate(outs):
            out[:, columns] = value[n * size:(n + 1) * size].astype(out.dtype)

    loop(coef.shape[1] // COLUMN_TILE, tile)


def multiply(at, sources, coef, pieces):
    depth = len(sources)
    rows, inner = sources[0].shape
    half = rows // 2
    columns = coef.shape[1]
    quarter = len(pieces) * half // 4
    out = jax.ShapeDtypeStruct((quarter, columns), jnp.bfloat16)
    taken = jax.ShapeDtypeStruct((len(pieces) * half, inner), jnp.bfloat16)
    return pl.pallas_call(
        functools.partial(multiply_kernel, depth=depth, pieces=pieces, half=half),
        out_shape=(out,) * 4,
        in_specs=[SMEM] + [ANY] * len(sources) + [VMEM],
        out_specs=(VMEM,) * 4,
        scratch_shapes=[pltpu.VMEM(taken.shape, taken.dtype), pltpu.SemaphoreType.DMA((len(pieces),))],
        compiler_params=pltpu.CompilerParams(vmem_limit_bytes=room(coef, taken, out, out, out, out)),
        cost_estimate=pl.CostEstimate(
            flops=2 * taken.size * columns, transcendentals=0,
            bytes_accessed=2 * (inner * columns + taken.size + 4 * out.size)),
        name="multiply",
    )(at, *sources, coef)


def per_device(blocks, pairs, counts, owned_blocks, occ_coef, vir_coef):
    groups = lax.axis_size("ao")
    depth = lax.axis_size("aux")
    me = lax.axis_index("ao")
    layer = lax.axis_index("aux")
    core, chip = me % 2, me // 2
    chips = groups // 2
    bits = chips.bit_length() - 1
    slots, aux_depth, _, width = blocks.shape
    occupied = occ_coef.shape[1]
    per_owner = owned_blocks.shape[0]

    vir_other = swap_ao(vir_coef, 1)

    ints = jnp.concatenate([pairs.reshape(-1), counts, owned_blocks])
    ints = jnp.pad(ints, (0, -ints.shape[0] % 128))[None, None, :]
    all_ints = lax.all_gather(ints, "ao", axis=0, tiled=True)
    occ_all = lax.all_gather(occ_coef, "ao", axis=0, tiled=True)
    occ_at, dest, pack, pick, load = make_plan(me, all_ints, groups, slots, per_owner)

    slab = jnp.einsum("sim,spmn->spin", occ_all[occ_at], blocks, preferred_element_type=jnp.float32)
    in_use = jnp.arange(slots, dtype=jnp.int32) < counts[0]
    slab = jnp.where(in_use[:, None, None, None], slab, 0.0).astype(jnp.bfloat16)
    rows = aux_depth // 2 * occupied
    slab = slab.reshape(slots, 2, rows, width)
    mine = lax.dynamic_index_in_dim(slab, core, 1, keepdims=False)
    theirs = swap_ao(lax.dynamic_index_in_dim(slab, 1 - core, 1, keepdims=False), 1)
    at = jnp.stack([chip, layer]).astype(jnp.int32)

    orders = [list(range(bits)), list(range(bits))[::-1]]
    flags = [[1 << b for b in order] for order in orders]
    send = [[r for r in range(chips) if r & flags[q][0]] for q in range(2)]
    keep = [[r for r in range(chips) if not r & flags[q][0]] for q in range(2)]
    pieces = [(q, r) for part in (send, keep) for q in range(2) for r in part[q]]

    def rest(cap, used_blocks, *operands):
        return transform(cap, used_blocks, *operands)

    def transform(cap, used_blocks, mine, theirs, dest, pack, pick, vir_own, vir_other):
        outgoing = pack_slots(mine, theirs, pack, chips, cap)
        coef = pick_blocks(vir_own, vir_other, pick, used_blocks, width)
        exchanged = []
        for g in range(len(GROUPS)):
            part = outgoing[g * (chips - 1):(g + 1) * (chips - 1)]
            exchanged.append([])
            for rel, x in enumerate(part, 1):
                exchanged[g].append(swap_ao(x, 2 * rel))
        chunks = []
        row0 = 0
        for g, group in enumerate(GROUPS):
            sizes = [rows * quarters // QUARTERS for quarters in group]
            chunks += sum_slots(mine, theirs, exchanged[g], dest, used_blocks, row0, sizes)
            row0 += sum(sizes)
        gathered = []
        for own in chunks:
            pieces_of = {0: own}
            for b in reversed(range(depth.bit_length() - 1)):
                for rel in list(pieces_of):
                    pieces_of[rel | 1 << b] = swap_aux(pieces_of[rel], 1 << b)
            gathered.append([pieces_of[rel] for rel in range(depth)])

        outs = []
        for c in range(len(chunks)):
            half = chunks[c].shape[0] // 2
            product = multiply(at, gathered[c], coef, pieces)
            out, held = product[:2], product[2:]
            held = [{r: held[q][n * half:(n + 1) * half] for n, r in enumerate(keep[q])} for q in range(2)]
            for b in range(bits):
                got = []
                for q in range(2):
                    got.append(swap_ao(out[q], 2 * flags[q][b]))
                total = [
                    {r: held[q][r].astype(jnp.float32) + got[q][n * half:(n + 1) * half].astype(jnp.float32)
                     for n, r in enumerate(sorted(held[q]))}
                    for q in range(2)
                ]
                if b + 1 < bits:
                    flag = [flags[q][b + 1] for q in range(2)]
                    out = [
                        jnp.concatenate([total[q][r] for r in sorted(total[q]) if r & flag[q]]).astype(jnp.bfloat16)
                        for q in range(2)
                    ]
                    held = [{r: v for r, v in total[q].items() if not r & flag[q]} for q in range(2)]
            outs += [total[q][0].astype(jnp.bfloat16) for q in range(2)]
        return jnp.concatenate(outs, axis=0)

    most, both = 2 * per_owner, 2 * slots
    plans = [(slots, most // 2), (both * 3 // 4, most * 7 // 10), (both, most)]
    sent, filled = load[chips * chips], load[chips * chips + 1]
    level = sum(
        1 - ((sent <= cap) & (filled <= used)).astype(jnp.int32) for cap, used in plans[:-1])
    result = lax.switch(
        level, [functools.partial(rest, *plan) for plan in plans],
        mine, theirs, dest, pack, pick, vir_coef, vir_other)
    return result.reshape(aux_depth // 2, occupied, vir_coef.shape[1])


def solution(mesh):
    in_specs = (
        P("ao", "aux", None, None),
        P("ao", None),
        P("ao"),
        P("ao"),
        P("ao", None, None),
        P("ao", "aux"),
    )
    out_specs = P("ao", None, "aux")
    return jax.shard_map(
        per_device, mesh=mesh, in_specs=in_specs, out_specs=out_specs, check_vma=False
    )
```
